512 devices in a mesh: vocab: 128 (over z, y, core), width: 4 (over x).
Axes of the slice: x: 4, y: 4, z: 16, core: 2. Of those that a mesh axis runs over, the one named last changes fastest.
Arguments:
- qwen_hidden: bfloat16 [256, 8192], P('vocab', 'width'), may hold values from -96 to 96
- qwen_next_hidden: bfloat16 [256, 8192], P('vocab', 'width'), may hold values from -96 to 96
- llama_hidden: bfloat16 [256, 8192], P('vocab', 'width'), may hold values from -96 to 96
- llama_next_hidden: bfloat16 [256, 8192], P('vocab', 'width'), may hold values from -96 to 96
- qwen_head: bfloat16 [81920, 8192], P('vocab', 'width'), may hold values from -0.198873782 to 0.198873782
- llama_head: bfloat16 [65536, 8192], P('vocab', 'width'), may hold values from -0.198873782 to 0.198873782
- align_weights: bfloat16 [4, 128, 128], replicated, may hold values from 0 to 1, as said below
- qwen_links: int32 [1280, 3], replicated, may hold values from 0 to 1023, as said below
- llama_links: int32 [1024, 3], replicated, may hold values from 0 to 1023, as said below
- union_order: int32 [1024], replicated, may hold values from 0 to 1023, each once
- chosen: int32 [256], P('vocab'), may hold values from 0 to 131071
- model_weight: float32 [2], replicated, may hold values from 0.25 to 1
Outputs:
- next_logprob: float32 [256, 131072], P(None, ('vocab', 'width'))
- chosen_loglik: float32 [256], P('vocab')
The draws below stay inside these ranges and needn't reach their ends.
Inputs may be any that keep to these rules, and one draw needn't show every extreme that they name: `qwen_links`: each row is (source block, union block, alignment matrix). Each of the 640 source blocks stands in exactly 2 rows; union blocks are below 1024; alignment matrices below 4. `llama_links`: each row is (source block, union block, alignment matrix). Each of the 512 source blocks stands in exactly 2 rows; every union block stands in exactly one row; alignment matrices below 4. `align_weights`: all entries positive; every row of every matrix sums to one up to bfloat16 rounding.
All inputs are finite; a program needn't handle non-finite values.
Results may differ from the reference program's by a relative error of at most 0.00075.
Values may be sent and summed in bfloat16 or wider, within the bound.
A program may use at most 64 MiB of HBM per device.

```python
import jax
import jax.numpy as jnp

D = 8192
BLOCK = 128
FAN = 2
KINDS = 4
ROWS = 256
QBLOCKS = 640
LBLOCKS = 512
UBLOCKS = 1024
QVOCAB = 81920
LVOCAB = 65536
UNION = 131072


def head_row(key, tag, row_id):
    row_key = jax.random.fold_in(jax.random.fold_in(key, tag), row_id)
    values = jnp.clip(jax.random.normal(row_key, (D,), jnp.float32), -6.0, 6.0)
    return values * (3.0 / jnp.sqrt(D * 1.0))


def head_matrix(key, tag, count):
    return jax.vmap(lambda row_id: head_row(key, tag, row_id))(jnp.arange(count, dtype=jnp.int32))


def hidden_rows(key, own_tag, head_tag, vocab_size):
    own_key = jax.random.fold_in(key, own_tag)
    values = jnp.clip(jax.random.normal(own_key, (ROWS, D), jnp.float32), -6.0, 6.0)
    shared_order = jax.random.permutation(jax.random.fold_in(key, 99), ROWS)
    slot = own_tag - 11
    picks = jax.lax.dynamic_slice_in_dim(shared_order, slot * 2, 2)
    leading = jax.random.randint(jax.random.fold_in(own_key, 4), (2,), 0, vocab_size)
    offsets = jax.random.randint(jax.random.fold_in(own_key, 5), (2,), 1, vocab_size)
    trailing = (leading + offsets) % vocab_size
    strengths = jnp.array([260.0, 150.0], jnp.float32)
    former = jax.vmap(lambda row_id: head_row(key, head_tag, row_id))(leading)
    latter = jax.vmap(lambda row_id: head_row(key, head_tag, row_id))(trailing)
    aligned = strengths[:, None] * former / jnp.sum(former * former, axis=1, keepdims=True)
    aligned = aligned + (strengths - 2.0)[:, None] * latter / jnp.sum(latter * latter, axis=1, keepdims=True)
    values = values.at[picks].set(aligned)
    return jnp.clip(values, -96.0, 96.0)


def link_table(key, blocks, skewed):
    count = blocks * FAN
    sources = jnp.arange(count, dtype=jnp.int32) // FAN
    if skewed:
        former = jax.random.randint(jax.random.fold_in(key, 1), (count,), 0, UBLOCKS)
        latter = jax.random.randint(jax.random.fold_in(key, 2), (count,), 0, UBLOCKS)
        relabel = jax.random.permutation(jax.random.fold_in(key, 3), UBLOCKS).astype(jnp.int32)
        unions = relabel[jnp.minimum(former, latter)]
    else:
        unions = jax.random.permutation(jax.random.fold_in(key, 3), UBLOCKS).astype(jnp.int32)
    kinds = jax.random.randint(jax.random.fold_in(key, 4), (count,), 0, KINDS).astype(jnp.int32)
    order = jax.random.permutation(jax.random.fold_in(key, 5), count)
    return jnp.stack([sources, unions.astype(jnp.int32), kinds], axis=1)[order].astype(jnp.int32)


def draw_qwen_head(key, part):
    return head_matrix(key, 1, QVOCAB).astype(jnp.bfloat16)


def draw_llama_head(key, part):
    return head_matrix(key, 2, LVOCAB).astype(jnp.bfloat16)


def draw_qwen_hidden(key, part):
    return hidden_rows(key, 11, 1, QVOCAB).astype(jnp.bfloat16)


def draw_qwen_next_hidden(key, part):
    return hidden_rows(key, 12, 1, QVOCAB).astype(jnp.bfloat16)


def draw_llama_hidden(key, part):
    return hidden_rows(key, 13, 2, LVOCAB).astype(jnp.bfloat16)


def draw_llama_next_hidden(key, part):
    return hidden_rows(key, 14, 2, LVOCAB).astype(jnp.bfloat16)


def draw_align_weights(key, part):
    weight_key = jax.random.fold_in(key, 21)
    raw = jax.random.uniform(weight_key, (KINDS, BLOCK, BLOCK), jnp.float32, 0.2, 2.2)
    raw = raw + 8.0 * jnp.eye(BLOCK, dtype=jnp.float32)[None, :, :]
    return (raw / jnp.sum(raw, axis=2, keepdims=True)).astype(jnp.bfloat16)


def draw_qwen_links(key, part):
    return link_table(jax.random.fold_in(key, 31), QBLOCKS, True)


def draw_llama_links(key, part):
    return link_table(jax.random.fold_in(key, 32), LBLOCKS, False)


def with_ends(values, stream_key, least, largest):
    extent = values.shape
    spot = [jax.random.randint(jax.random.fold_in(stream_key, axis), (), 0, extent[axis]) for axis in range(len(extent))]
    values = values.at[tuple(spot)].set(least)
    longest = extent.index(max(extent))
    spot[longest] = (spot[longest] + 1) % extent[longest]
    return values.at[tuple(spot)].set(largest)


def setup_inputs(seed: int = 0) -> dict:
    keys = jax.random.split(jax.random.key(seed), 13)
    return {
        "qwen_hidden": draw_qwen_hidden(jax.random.fold_in(keys[12], 71), 0),
        "qwen_next_hidden": draw_qwen_next_hidden(jax.random.fold_in(keys[12], 71), 0),
        "llama_hidden": draw_llama_hidden(jax.random.fold_in(keys[12], 71), 0),
        "llama_next_hidden": draw_llama_next_hidden(jax.random.fold_in(keys[12], 71), 0),
        "qwen_head": draw_qwen_head(jax.random.fold_in(keys[12], 71), 0),
        "llama_head": draw_llama_head(jax.random.fold_in(keys[12], 71), 0),
        "align_weights": draw_align_weights(jax.random.fold_in(keys[12], 71), 0),
        "qwen_links": draw_qwen_links(jax.random.fold_in(keys[12], 71), 0),
        "llama_links": draw_llama_links(jax.random.fold_in(keys[12], 71), 0),
        "union_order": jax.random.permutation(keys[9], UBLOCKS).astype(jnp.int32),
        "chosen": with_ends(jax.random.randint(keys[10], (ROWS,), 0, UNION), jax.random.fold_in(keys[10], 1), 0, UNION - 1).astype(jnp.int32),
        "model_weight": jnp.clip(jax.random.uniform(keys[11], (2,), jnp.float32, 0.25, 1.0), 0.25, 1.0),
    }


SMOOTHING = 0.01


def model_union(hidden, head, align_weights, links):
    logits = jnp.dot(hidden, head.T, preferred_element_type=jnp.float32)
    total_lse = jax.nn.logsumexp(logits, axis=1, keepdims=True)
    probs = jnp.exp(logits - total_lse).astype(jnp.bfloat16)
    blocks = probs.reshape(probs.shape[0], -1, BLOCK)
    picked = blocks[:, links[:, 0], :].astype(jnp.float32)
    summed = jnp.zeros(picked.shape, jnp.float32)
    for kind_index in range(KINDS):
        keeper = (links[:, 2] == kind_index).astype(jnp.float32)[None, :, None]
        matrix = align_weights[kind_index].astype(jnp.float32)
        summed = summed + jnp.einsum("reb,bc->rec", picked * keeper, matrix)
    spread = jax.ops.segment_sum(jnp.transpose(summed, (1, 0, 2)), links[:, 1], num_segments=UBLOCKS)
    spread = spread * (1.0 / FAN)
    return jnp.transpose(spread, (1, 0, 2)).reshape(picked.shape[0], UBLOCKS * BLOCK)


def reference(qwen_hidden, qwen_next_hidden, llama_hidden, llama_next_hidden, qwen_head, llama_head, align_weights, qwen_links, llama_links, union_order, chosen, model_weight):
    prior = model_weight / (model_weight[0] + model_weight[1])
    row_index = jnp.arange(ROWS, dtype=jnp.int32)
    uniform_part = SMOOTHING / (UBLOCKS * BLOCK)
    qwen_first = model_union(qwen_hidden, qwen_head, align_weights, qwen_links)
    llama_first = model_union(llama_hidden, llama_head, align_weights, llama_links)
    qwen_mass = prior[0] * ((1.0 - SMOOTHING) * qwen_first[row_index, chosen] + uniform_part)
    llama_mass = prior[1] * ((1.0 - SMOOTHING) * llama_first[row_index, chosen] + uniform_part)
    together = qwen_mass + llama_mass
    chosen_loglik = jnp.log(together)
    qwen_second = model_union(qwen_next_hidden, qwen_head, align_weights, qwen_links)
    llama_second = model_union(llama_next_hidden, llama_head, align_weights, llama_links)
    mixed = (qwen_mass / together)[:, None] * qwen_second + (llama_mass / together)[:, None] * llama_second
    ordered = mixed.reshape(ROWS, UBLOCKS, BLOCK)[:, union_order, :].reshape(ROWS, UBLOCKS * BLOCK)
    return jnp.log((1.0 - SMOOTHING) * ordered + uniform_part), chosen_loglik
```

```python
import functools

import jax
import jax.numpy as jnp
from jax import lax
from jax.experimental import pallas as pl
from jax.experimental.pallas import tpu as pltpu
from jax.sharding import Mesh
from jax.sharding import PartitionSpec as P

BLOCK = 128
QB_DEV = 5
LB_DEV = 4
B_DEV = QB_DEV + LB_DEV
KINDS = 4
UBLOCKS = 1024
SMOOTHING = 0.01
UNIFORM = SMOOTHING / (UBLOCKS * BLOCK)
VOCAB = ("vocab_0", "vocab_1", "vocab_2")
PLANE = ("vocab_0", "vocab_1")
GROUP = ("vocab_1", "vocab_2")


def positions_of(union_order, blocks):
    places = jnp.arange(UBLOCKS, dtype=jnp.int32)
    return jnp.sum(jnp.where(union_order[None, :] == blocks[:, None], places[None, :], 0), axis=1)


def link_codes(links, union_order, blocks):
    codes = positions_of(union_order, links[:, 1]) * KINDS + links[:, 2]
    hit = links[:, 0][None, :] == jnp.arange(blocks, dtype=jnp.int32)[:, None]
    low = jnp.min(jnp.where(hit, codes[None, :], UBLOCKS * KINDS), axis=1)
    high = jnp.max(jnp.where(hit, codes[None, :], -1), axis=1)
    return low, high


def three_parts(value):
    first = lax.reduce_precision(value, 8, 7)
    rest = value - first
    second = lax.reduce_precision(rest, 8, 7)
    third = lax.reduce_precision(rest - second, 8, 7)
    return [part.astype(jnp.bfloat16) for part in (first, second, third)]


def chosen_codes(chosen):
    block = chosen // BLOCK
    codes = jnp.stack([block // 32, block % 32, chosen % BLOCK], axis=1)
    return jnp.pad(codes.astype(jnp.bfloat16), ((0, 0), (0, BLOCK - 3)))


def gathered_tiles(hidden_cat, chosen):
    rows, columns = hidden_cat.shape
    parts = hidden_cat.reshape(rows, 8, columns // 8).transpose(1, 0, 2)
    codes = jnp.broadcast_to(chosen_codes(chosen)[None], (8, rows, BLOCK))
    tile = lax.all_to_all(jnp.concatenate([parts, codes], axis=2), GROUP, 0, 0, tiled=True)
    tile = tile.reshape(8 * rows, -1)
    tiles = lax.all_gather(tile, "vocab_1")
    tiles = lax.all_gather(tiles, "vocab_0")
    return lax.all_gather(tiles, "vocab_2", axis=2)


def partial_logits(tiles, qwen_head, llama_head):
    chunk = tiles.shape[-1] - BLOCK
    found = []
    for tensor in range(4):
        head = qwen_head if tensor < 2 else llama_head
        total = 0.0
        for half in range(2):
            place = tensor * 2 + half
            rows = tiles[:, place // 2, place % 2, :, :chunk].reshape(-1, chunk)
            total = total + lax.dot_general(
                rows,
                head[:, half * chunk : (half + 1) * chunk],
                (((1,), (1,)), ((), ())),
                preferred_element_type=jnp.float32,
            )
        found.append(total)
    first = jnp.concatenate([found[0], found[2]], axis=1)
    second = jnp.concatenate([found[1], found[3]], axis=1)
    return jnp.stack([first, second])


def width_summed(partial):
    steps, rows, entries = partial.shape
    split = jnp.moveaxis(partial.reshape(steps, rows // 4, 4, entries), 2, 0)
    return jnp.sum(lax.all_to_all(split, "width", 0, 0, tiled=True), axis=0)


def row_message(logits, chosen_pos, chosen_col, own_low, own_high, align_weights):
    rows = logits.shape[1]
    q_cols = QB_DEV * BLOCK
    models = (slice(0, q_cols), slice(q_cols, B_DEV * BLOCK))
    one_hot = (chosen_col[:, None] == jnp.arange(BLOCK, dtype=jnp.int32)[None, :]).astype(jnp.bfloat16)
    columns = jnp.einsum("rj,kij->kri", one_hot, align_weights, preferred_element_type=jnp.float32)
    weight = jnp.zeros((rows, B_DEV, BLOCK), jnp.float32)
    for kind in range(KINDS):
        code = (chosen_pos * KINDS + kind)[:, None]
        count = (own_low[None, :] == code).astype(jnp.float32) + (own_high[None, :] == code).astype(jnp.float32)
        weight = weight + count[:, :, None] * columns[kind][:, None, :]
    weight = weight.reshape(rows, B_DEV * BLOCK)
    values, terms = [], []
    for cols in models:
        part = logits[0, :, cols]
        top = jnp.max(part, axis=1, keepdims=True)
        powers = jnp.exp(part - top)
        values += [top, jnp.sum(powers, 1, keepdims=True), jnp.sum(powers * weight[:, cols], 1, keepdims=True)]
    for cols in models:
        part = logits[1, :, cols]
        top = jnp.max(part, axis=1, keepdims=True)
        powers = jnp.exp(part - top)
        values += [top, jnp.sum(powers, 1, keepdims=True)]
        terms.append(powers.astype(jnp.bfloat16))
    parts = three_parts(jnp.concatenate(values, axis=1))
    blank = jnp.zeros((rows, BLOCK - 30), jnp.bfloat16)
    return jnp.concatenate([*terms, *parts, blank], axis=1)


def rescaled(tops, sums):
    factor = jnp.exp(tops - jnp.max(tops))
    return factor, jnp.sum(factor * sums)


def row_scales(message, model_weight):
    stats = message[:, B_DEV * BLOCK :].astype(jnp.float32)
    stats = stats[:, 0:10] + stats[:, 10:20] + stats[:, 20:30]
    prior = model_weight / (model_weight[0] + model_weight[1])
    masses = []
    for model in range(2):
        factor, total = rescaled(stats[:, 3 * model], stats[:, 3 * model + 1])
        value = 0.5 * jnp.sum(factor * stats[:, 3 * model + 2]) / total
        masses.append(prior[model] * ((1.0 - SMOOTHING) * value + UNIFORM))
    together = masses[0] + masses[1]
    scales = []
    for model in range(2):
        factor, total = rescaled(stats[:, 6 + 2 * model], stats[:, 7 + 2 * model])
        scales.append((masses[model] / together) * 0.5 * factor / total)
    return scales, jnp.log(together)


def map_kernel(low_ref, high_ref, terms_ref, weights_ref, out_ref):
    core = lax.axis_index("vocab_2")
    half = out_ref.shape[0]
    spot = lax.broadcasted_iota(jnp.int32, (half, BLOCK), 0)
    first = (16 * (spot // 4) + 8 * core + 2 * (spot % 4)) * KINDS
    for t in range(2):
        mixed = jnp.zeros((half, BLOCK), jnp.float32)
        for kind in range(KINDS):
            code = first + (t * KINDS + kind)
            total = jnp.zeros((half, BLOCK), jnp.float32)
            for b in range(B_DEV):
                hits = jnp.where(low_ref[b : b + 1, :] == code, 1.0, 0.0) + jnp.where(
                    high_ref[b : b + 1, :] == code, 1.0, 0.0
                )
                total += jnp.dot(
                    hits.astype(jnp.bfloat16),
                    terms_ref[:, b * BLOCK : (b + 1) * BLOCK],
                    preferred_element_type=jnp.float32,
                )
            mixed += jnp.dot(
                total.astype(jnp.bfloat16), weights_ref[kind], preferred_element_type=jnp.float32
            )
        out_ref[:, t * BLOCK : (t + 1) * BLOCK] = mixed.astype(out_ref.dtype)


def mapped(low, high, terms, align_weights):
    return pl.pallas_call(
        map_kernel,
        out_shape=jax.ShapeDtypeStruct((UBLOCKS // 4, 2 * BLOCK), jnp.bfloat16),
    )(low, high, terms, align_weights)


def by_source(codes, per_device):
    return codes.reshape(-1, 2, per_device).transpose(2, 1, 0).reshape(per_device, -1)


def local(
    qwen_hidden,
    qwen_next_hidden,
    llama_hidden,
    llama_next_hidden,
    qwen_head,
    llama_head,
    align_weights,
    qwen_links,
    llama_links,
    union_order,
    chosen,
    model_weight,
):
    core = lax.axis_index("vocab_2")
    width = lax.axis_index("width")
    owner = lax.axis_index(VOCAB)
    hidden_cat = jnp.concatenate(
        [qwen_hidden, qwen_next_hidden, llama_hidden, llama_next_hidden], axis=1
    )
    tiles = gathered_tiles(hidden_cat, chosen)
    codes = tiles[:, 0, 0, :, -BLOCK:][:, :, :3].astype(jnp.int32).reshape(-1, 4, 3)
    codes = lax.dynamic_index_in_dim(codes, width, 1, keepdims=False)
    chosen_pos = positions_of(union_order, codes[:, 0] * 32 + codes[:, 1])
    q_low, q_high = link_codes(qwen_links, union_order, qwen_links.shape[0] // 2)
    l_low, l_high = link_codes(llama_links, union_order, llama_links.shape[0] // 2)
    own_low, own_high = (
        jnp.concatenate(
            [
                lax.dynamic_slice(q, (owner * QB_DEV,), (QB_DEV,)),
                lax.dynamic_slice(l, (owner * LB_DEV,), (LB_DEV,)),
            ]
        )
        for q, l in ((q_low, l_low), (q_high, l_high))
    )
    low, high = (
        jnp.concatenate([by_source(q, QB_DEV), by_source(l, LB_DEV)])
        for q, l in ((q_low, l_low), (q_high, l_high))
    )
    logits = width_summed(partial_logits(tiles, qwen_head, llama_head))
    message = row_message(logits, chosen_pos, codes[:, 2], own_low, own_high, align_weights)
    message = lax.all_to_all(message, PLANE, 0, 0, tiled=True)
    message = lax.all_gather(message, "vocab_2", axis=0, tiled=True)
    (q_scale, l_scale), loglik = row_scales(message, model_weight)
    q_cols = QB_DEV * BLOCK
    terms = message[:, : B_DEV * BLOCK].astype(jnp.float32)
    terms = jnp.concatenate(
        [terms[:, :q_cols] * q_scale[:, None], terms[:, q_cols:] * l_scale[:, None]], axis=1
    ).astype(jnp.bfloat16)
    mixed = mapped(low, high, terms, align_weights)
    owned = lax.all_to_all(mixed, ("vocab_0", "vocab_1", "width"), 0, 0, tiled=True)
    next_logprob = jnp.log((1.0 - SMOOTHING) * owned.astype(jnp.float32) + UNIFORM)
    logliks = lax.all_gather(loglik, "width")
    return next_logprob, lax.dynamic_slice(logliks, (2 * core,), (2,))


def solution(mesh):
    torus = Mesh(
        mesh.devices.reshape(16, 4, 2, mesh.shape["width"]),
        ("vocab_0", "vocab_1", "vocab_2", "width"),
    )
    return jax.shard_map(
        local,
        mesh=torus,
        in_specs=(*[P(VOCAB, "width")] * 6, P(), P(), P(), P(), P(VOCAB), P()),
        out_specs=(P(None, (*VOCAB, "width")), P(VOCAB)),
        check_vma=False,
    )
```

```python
import functools

import jax
import jax.numpy as jnp
from jax import lax
from jax.experimental import pallas as pl
from jax.experimental.pallas import tpu as pltpu
from jax.sharding import Mesh
from jax.sharding import PartitionSpec as P

BLOCK = 128
QB_DEV = 5
LB_DEV = 4
B_DEV = QB_DEV + LB_DEV
KINDS = 4
UBLOCKS = 1024
SMOOTHING = 0.01
UNIFORM = SMOOTHING / (UBLOCKS * BLOCK)
VOCAB = ("vocab_0", "vocab_1", "vocab_2")
PLANE = ("vocab_0", "vocab_1")
GROUP = ("vocab_1", "vocab_2")


def positions_of(union_order, blocks):
    places = jnp.arange(UBLOCKS, dtype=jnp.int32)
    return jnp.sum(jnp.where(union_order[None, :] == blocks[:, None], places[None, :], 0), axis=1)


def link_codes(links, union_order, blocks):
    codes = positions_of(union_order, links[:, 1]) * KINDS + links[:, 2]
    hit = links[:, 0][None, :] == jnp.arange(blocks, dtype=jnp.int32)[:, None]
    low = jnp.min(jnp.where(hit, codes[None, :], UBLOCKS * KINDS), axis=1)
    high = jnp.max(jnp.where(hit, codes[None, :], -1), axis=1)
    return low, high


def three_parts(value):
    first = lax.reduce_precision(value, 8, 7)
    rest = value - first
    second = lax.reduce_precision(rest, 8, 7)
    third = lax.reduce_precision(rest - second, 8, 7)
    return [part.astype(jnp.bfloat16) for part in (first, second, third)]


def chosen_codes(chosen):
    block = chosen // BLOCK
    codes = jnp.stack([block // 32, block % 32, chosen % BLOCK], axis=1)
    return jnp.pad(codes.astype(jnp.bfloat16), ((0, 0), (0, BLOCK - 3)))


def column_tile(hidden_cat, chosen):
    rows, columns = hidden_cat.shape
    parts = hidden_cat.reshape(rows, 8, columns // 8).transpose(1, 0, 2)
    codes = jnp.broadcast_to(chosen_codes(chosen)[None], (8, rows, BLOCK))
    tile = lax.all_to_all(jnp.concatenate([parts, codes], axis=2), GROUP, 0, 0, tiled=True)
    tile = tile.reshape(8 * rows, -1)
    return tile[:, :-BLOCK], tile[:, -BLOCK:]


def chunk_tensor(y, k):
    return lax.rem(y + 4 - k, 4)


def logits_kernel(
    tile_ref,
    code_ref,
    q_head_ref,
    l_head_ref,
    out_ref,
    codes_ref,
    held,
    codes,
    q_head,
    l_head,
    found,
    parts,
    sums,
    head_sem,
    y_send,
    y_recv,
    z_send,
    z_recv,
    code_send,
    code_recv,
    core_send,
    core_recv,
    x_send,
    x_recv,
):
    z, y, c, x = (lax.axis_index(name) for name in ("vocab_0", "vocab_1", "vocab_2", "width"))
    other = 1 - c
    z_next = (lax.rem(z + 1, 16), lax.rem(z + 15, 16))
    x_next = (lax.rem(x + 1, 4), lax.rem(x + 3, 4))
    chunk = tile_ref.shape[1]
    q_rows = q_head_ref.shape[0]

    def to(src, dst, send, recv, axis, index):
        return pltpu.make_async_remote_copy(
            src_ref=src,
            dst_ref=dst,
            send_sem=send,
            recv_sem=recv,
            device_id={axis: index},
            device_id_type=pl.DeviceIdType.MESH,
        )

    def plane(way, step):
        return lax.rem(z + 16 - step, 16) if way == 0 else lax.rem(z + step, 16)

    def pair(group):
        return lax.rem(z + 16 - group, 16), lax.rem(z + jnp.where(group == 8, 0, group), 16)

    def z_copy(way, k, step, src=None):
        place = held.at[plane(way, step - 1), c, chunk_tensor(y, k)]
        return to(
            place if src is None else src,
            place,
            z_send.at[way, k, step],
            z_recv.at[way, k, step],
            "vocab_0",
            z_next[way],
        )

    def z_arrival(way, k, step):
        place = held.at[plane(way, step), c, chunk_tensor(y, k)]
        return to(place, place, z_send.at[way, k, step], z_recv.at[way, k, step], "vocab_0", z_next[way])

    def code_copy(way, step, at):
        place = codes.at[plane(way, at)]
        return to(
            place, place, code_send.at[way, step], code_recv.at[way, step], "vocab_0", z_next[way]
        )

    def core_copy(way, step, at, core):
        place = held.at[at, core]
        return to(place, place, core_send.at[way, step], core_recv.at[way, step], "vocab_2", other)

    def x_copy(hop, way, group, src):
        return to(
            src,
            sums.at[hop, way, group],
            x_send.at[hop, way, group],
            x_recv.at[hop, way, group],
            "width",
            x_next[way],
        )

    def x_class(way, hop):
        return lax.rem(x + 7 - hop, 4) if way == 0 else lax.rem(x + 1 + hop, 4)

    head_copies = (
        pltpu.make_async_copy(q_head_ref, q_head, head_sem.at[0]),
        pltpu.make_async_copy(l_head_ref, l_head, head_sem.at[1]),
    )
    for copy in head_copies:
        copy.start()
    barrier = pltpu.get_barrier_semaphore()
    peers = [("vocab_0", z_next[0]), ("vocab_0", z_next[1]), ("vocab_2", other)]
    peers += [("vocab_1", lax.rem(y + step, 4)) for step in (1, 2, 3)]
    peers += [("width", x_next[0]), ("width", x_next[1])]
    for axis, index in peers:
        pl.semaphore_signal(
            barrier, inc=1, device_id={axis: index}, device_id_type=pl.DeviceIdType.MESH
        )
    pl.semaphore_wait(barrier, len(peers))

    y_copies = [
        to(tile_ref, held.at[z, c, y], y_send.at[k], y_recv.at[k], "vocab_1", lax.rem(y + k + 1, 4))
        for k in range(3)
    ]
    for copy in y_copies:
        copy.start()
    for way in range(2):
        z_copy(way, 0, 1, tile_ref).start()
        to(
            code_ref,
            codes.at[z],
            code_send.at[way, 1],
            code_recv.at[way, 1],
            "vocab_0",
            z_next[way],
        ).start()
    held[z, c, y] = tile_ref[...]
    codes[z] = code_ref[...]
    for k in range(1, 4):
        place = held.at[z, c, chunk_tensor(y, k)]
        to(place, place, y_send.at[k - 1], y_recv.at[k - 1], "vocab_1", y).wait_recv()
        for way in range(2):
            z_copy(way, k, 1).start()
    core_copy(1, 8, z, c).start()
    for copy in head_copies:
        copy.wait()

    def step(it, carry):
        for k in range(4):
            for way in range(2):
                last = 8 if (k < 2) == (way == 0) else 7

                @pl.when(it <= last)
                def _():
                    z_arrival(way, k, it).wait_recv()

                @pl.when(it < last)
                def _():
                    z_copy(way, k, it + 1).start()

        for way in range(2):
            last = 8 - way

            @pl.when(it <= last)
            def _():
                code_copy(way, it, it).wait_recv()
                core_copy(way, it, plane(way, it), c).start()

            @pl.when(it < last)
            def _():
                code_copy(way, it + 1, it).start()

        group = it - 1

        @pl.when((group >= 1) & (group <= 8))
        def _():
            low, high = pair(group)
            core_copy(0, group, low, other).wait_recv()
            core_copy(1, group, high, other).wait_recv()
            for model in range(2):
                head, first = (q_head, 0) if model == 0 else (l_head, q_rows)
                total = None
                for half in range(2):
                    rows = jnp.concatenate(
                        [held[at, half, 2 * model + s] for s in range(2) for at in (low, high)], axis=0
                    )
                    term = lax.dot_general(
                        rows,
                        head[:, half * chunk : (half + 1) * chunk],
                        (((1,), (1,)), ((), ())),
                        preferred_element_type=jnp.float32,
                    )
                    total = term if total is None else total + term
                for b in range(head.shape[0] // BLOCK):
                    found[first // BLOCK + b] = total[:, b * BLOCK : (b + 1) * BLOCK]
            for b in range(B_DEV):
                for s in range(2):
                    for turn in range(4):
                        rows = found[b, pl.ds(32 * s + turn, 8, stride=4), :]
                        parts[group, s, turn, :, b * BLOCK : (b + 1) * BLOCK] = rows
            for way in range(2):
                x_copy(0, way, group, parts.at[group, way, x_class(way, 0)]).start()

        for hop in (1, 2):
            group_h = it - 1 - hop

            @pl.when((group_h >= 1) & (group_h <= 8))
            def _():
                for way in range(2):
                    place = sums.at[hop - 1, way, group_h]
                    x_copy(hop - 1, way, group_h, place).wait_recv()
                    place[...] = place[...] + parts[group_h, way, x_class(way, hop)]
                    x_copy(hop, way, group_h, place).start()

        group_d = it - 4

        @pl.when((group_d >= 1) & (group_d <= 8))
        def _():
            low, high = pair(group_d)
            for way in range(2):
                place = sums.at[2, way, group_d]
                x_copy(2, way, group_d, place).wait_recv()
                total = place[...] + parts[group_d, way, x]
                out_ref[way, low] = total[0:4]
                out_ref[way, high] = total[4:8]

        return carry

    lax.fori_loop(1, 13, step, 0)
    codes_ref[...] = codes[...]

    for copy in y_copies:
        copy.wait_send()

    def drain(it, carry):
        for way in range(2):
            for k in range(4):
                last = 8 if (k < 2) == (way == 0) else 7

                @pl.when(it <= last)
                def _():
                    z_copy(way, k, it).wait_send()

            last = 8 - way

            @pl.when(it <= last)
            def _():
                code_copy(way, it, it).wait_send()

            core_copy(way, it, z, c).wait_send()
            for hop in range(3):
                x_copy(hop, way, it, sums.at[0, way, it]).wait_send()
        return carry

    lax.fori_loop(1, 9, drain, 0)


def reduced_logits(tile, code, q_head, l_head):
    rows, chunk = tile.shape
    entries = q_head.shape[0] + l_head.shape[0]
    vmem = pl.BlockSpec(memory_space=pltpu.VMEM)
    dma = pltpu.SemaphoreType.DMA
    return pl.pallas_call(
        logits_kernel,
        out_shape=(
            jax.ShapeDtypeStruct((2, 16, 4, entries), jnp.float32),
            jax.ShapeDtypeStruct((16, rows, BLOCK), jnp.bfloat16),
        ),
        in_specs=[vmem, vmem, *[pl.BlockSpec(memory_space=pltpu.HBM)] * 2],
        out_specs=(vmem, vmem),
        scratch_shapes=[
            pltpu.VMEM((16, 2, 4, rows, chunk), jnp.bfloat16),
            pltpu.VMEM((16, rows, BLOCK), jnp.bfloat16),
            pltpu.VMEM(q_head.shape, jnp.bfloat16),
            pltpu.VMEM(l_head.shape, jnp.bfloat16),
            pltpu.VMEM((B_DEV, 4 * rows, BLOCK), jnp.float32),
            pltpu.VMEM((9, 2, 4, 8, entries), jnp.float32),
            pltpu.VMEM((3, 2, 9, 8, entries), jnp.float32),
            dma((2,)),
            dma((3,)),
            dma((3,)),
            dma((2, 4, 9)),
            dma((2, 4, 9)),
            dma((2, 9)),
            dma((2, 9)),
            dma((2, 9)),
            dma((2, 9)),
            dma((3, 2, 9)),
            dma((3, 2, 9)),
        ],
        compiler_params=pltpu.CompilerParams(
            collective_id=0, has_side_effects=True, vmem_limit_bytes=40 * 1024 * 1024
        ),
        cost_estimate=pl.CostEstimate(flops=3 * 10**10, bytes_accessed=10**7, transcendentals=0),
    )(tile, code, q_head, l_head)


def row_message(logits, chosen_pos, chosen_col, own_low, own_high, align_weights):
    rows = logits.shape[1]
    q_cols = QB_DEV * BLOCK
    models = (slice(0, q_cols), slice(q_cols, B_DEV * BLOCK))
    one_hot = (chosen_col[:, None] == jnp.arange(BLOCK, dtype=jnp.int32)[None, :]).astype(jnp.bfloat16)
    columns = jnp.einsum("rj,kij->kri", one_hot, align_weights, preferred_element_type=jnp.float32)
    weight = jnp.zeros((rows, B_DEV, BLOCK), jnp.float32)
    for kind in range(KINDS):
        code = (chosen_pos * KINDS + kind)[:, None]
        count = (own_low[None, :] == code).astype(jnp.float32) + (own_high[None, :] == code).astype(jnp.float32)
        weight = weight + count[:, :, None] * columns[kind][:, None, :]
    weight = weight.reshape(rows, B_DEV * BLOCK)
    values, terms = [], []
    for cols in models:
        part = logits[0, :, cols]
        top = jnp.max(part, axis=1, keepdims=True)
        powers = jnp.exp(part - top)
        values += [top, jnp.sum(powers, 1, keepdims=True), jnp.sum(powers * weight[:, cols], 1, keepdims=True)]
    for cols in models:
        part = logits[1, :, cols]
        top = jnp.max(part, axis=1, keepdims=True)
        powers = jnp.exp(part - top)
        values += [top, jnp.sum(powers, 1, keepdims=True)]
        terms.append(powers.astype(jnp.bfloat16))
    parts = three_parts(jnp.concatenate(values, axis=1))
    blank = jnp.zeros((rows, BLOCK - 30), jnp.bfloat16)
    return jnp.concatenate([*terms, *parts, blank], axis=1)


def rescaled(tops, sums):
    factor = jnp.exp(tops - jnp.max(tops))
    return factor, jnp.sum(factor * sums)


def row_scales(message, model_weight):
    stats = message[:, B_DEV * BLOCK :].astype(jnp.float32)
    stats = stats[:, 0:10] + stats[:, 10:20] + stats[:, 20:30]
    prior = model_weight / (model_weight[0] + model_weight[1])
    masses = []
    for model in range(2):
        factor, total = rescaled(stats[:, 3 * model], stats[:, 3 * model + 1])
        value = 0.5 * jnp.sum(factor * stats[:, 3 * model + 2]) / total
        masses.append(prior[model] * ((1.0 - SMOOTHING) * value + UNIFORM))
    together = masses[0] + masses[1]
    scales = []
    for model in range(2):
        factor, total = rescaled(stats[:, 6 + 2 * model], stats[:, 7 + 2 * model])
        scales.append((masses[model] / together) * 0.5 * factor / total)
    return scales, jnp.log(together)


def map_kernel(low_ref, high_ref, terms_ref, weights_ref, out_ref):
    core = lax.axis_index("vocab_2")
    half = out_ref.shape[0]
    spot = lax.broadcasted_iota(jnp.int32, (half, BLOCK), 0)
    first = (16 * (spot // 4) + 8 * core + 2 * (spot % 4)) * KINDS
    for t in range(2):
        mixed = jnp.zeros((half, BLOCK), jnp.float32)
        for kind in range(KINDS):
            code = first + (t * KINDS + kind)
            total = jnp.zeros((half, BLOCK), jnp.float32)
            for b in range(B_DEV):
                hits = jnp.where(low_ref[b : b + 1, :] == code, 1.0, 0.0) + jnp.where(
                    high_ref[b : b + 1, :] == code, 1.0, 0.0
                )
                total += jnp.dot(
                    hits.astype(jnp.bfloat16),
                    terms_ref[:, b * BLOCK : (b + 1) * BLOCK],
                    preferred_element_type=jnp.float32,
                )
            mixed += jnp.dot(
                total.astype(jnp.bfloat16), weights_ref[kind], preferred_element_type=jnp.float32
            )
        out_ref[:, t * BLOCK : (t + 1) * BLOCK] = mixed.astype(out_ref.dtype)


def mapped(low, high, terms, align_weights):
    return pl.pallas_call(
        map_kernel,
        out_shape=jax.ShapeDtypeStruct((UBLOCKS // 4, 2 * BLOCK), jnp.bfloat16),
    )(low, high, terms, align_weights)


def by_source(codes, per_device):
    return codes.reshape(-1, 2, per_device).transpose(2, 1, 0).reshape(per_device, -1)


def local(
    qwen_hidden,
    qwen_next_hidden,
    llama_hidden,
    llama_next_hidden,
    qwen_head,
    llama_head,
    align_weights,
    qwen_links,
    llama_links,
    union_order,
    chosen,
    model_weight,
):
    core = lax.axis_index("vocab_2")
    width = lax.axis_index("width")
    owner = lax.axis_index(VOCAB)
    hidden_cat = jnp.concatenate(
        [qwen_hidden, qwen_next_hidden, llama_hidden, llama_next_hidden], axis=1
    )
    logits, codes = reduced_logits(*column_tile(hidden_cat, chosen), qwen_head, llama_head)
    logits = logits.reshape(2, -1, B_DEV * BLOCK)
    codes = codes[:, :, :3].astype(jnp.int32).reshape(-1, 4, 3)
    codes = lax.dynamic_index_in_dim(codes, width, 1, keepdims=False)
    chosen_pos = positions_of(union_order, codes[:, 0] * 32 + codes[:, 1])
    q_low, q_high = link_codes(qwen_links, union_order, qwen_links.shape[0] // 2)
    l_low, l_high = link_codes(llama_links, union_order, llama_links.shape[0] // 2)
    own_low, own_high = (
        jnp.concatenate(
            [
                lax.dynamic_slice(q, (owner * QB_DEV,), (QB_DEV,)),
                lax.dynamic_slice(l, (owner * LB_DEV,), (LB_DEV,)),
            ]
        )
        for q, l in ((q_low, l_low), (q_high, l_high))
    )
    low, high = (
        jnp.concatenate([by_source(q, QB_DEV), by_source(l, LB_DEV)])
        for q, l in ((q_low, l_low), (q_high, l_high))
    )
    message = row_message(logits, chosen_pos, codes[:, 2], own_low, own_high, align_weights)
    message = lax.all_to_all(message, PLANE, 0, 0, tiled=True)
    message = lax.all_gather(message, "vocab_2", axis=0, tiled=True)
    (q_scale, l_scale), loglik = row_scales(message, model_weight)
    q_cols = QB_DEV * BLOCK
    terms = message[:, : B_DEV * BLOCK].astype(jnp.float32)
    terms = jnp.concatenate(
        [terms[:, :q_cols] * q_scale[:, None], terms[:, q_cols:] * l_scale[:, None]], axis=1
    ).astype(jnp.bfloat16)
    mixed = mapped(low, high, terms, align_weights)
    owned = lax.all_to_all(mixed, ("vocab_0", "vocab_1", "width"), 0, 0, tiled=True)
    next_logprob = jnp.log((1.0 - SMOOTHING) * owned.astype(jnp.float32) + UNIFORM)
    logliks = lax.all_gather(loglik, "width")
    return next_logprob, lax.dynamic_slice(logliks, (2 * core,), (2,))


def solution(mesh):
    torus = Mesh(
        mesh.devices.reshape(16, 4, 2, mesh.shape["width"]),
        ("vocab_0", "vocab_1", "vocab_2", "width"),
    )
    return jax.shard_map(
        local,
        mesh=torus,
        in_specs=(*[P(VOCAB, "width")] * 6, P(), P(), P(), P(), P(VOCAB), P()),
        out_specs=(P(None, (*VOCAB, "width")), P(VOCAB)),
        check_vma=False,
    )
```

```python
import functools

import jax
import jax.numpy as jnp
from jax import lax
from jax.experimental import pallas as pl
from jax.experimental.pallas import tpu as pltpu
from jax.sharding import Mesh
from jax.sharding import PartitionSpec as P

BLOCK = 128
QB_DEV = 5
LB_DEV = 4
B_DEV = QB_DEV + LB_DEV
KINDS = 4
UBLOCKS = 1024
SMOOTHING = 0.01
UNIFORM = SMOOTHING / (UBLOCKS * BLOCK)
VOCAB = ("vocab_0", "vocab_1", "vocab_2")
PLANE = ("vocab_0", "vocab_1")
GROUP = ("vocab_1", "vocab_2")


def positions_of(union_order, blocks):
    places = jnp.arange(UBLOCKS, dtype=jnp.int32)
    return jnp.sum(jnp.where(union_order[None, :] == blocks[:, None], places[None, :], 0), axis=1)


def link_codes(links, union_order, blocks):
    codes = positions_of(union_order, links[:, 1]) * KINDS + links[:, 2]
    hit = links[:, 0][None, :] == jnp.arange(blocks, dtype=jnp.int32)[:, None]
    low = jnp.min(jnp.where(hit, codes[None, :], UBLOCKS * KINDS), axis=1)
    high = jnp.max(jnp.where(hit, codes[None, :], -1), axis=1)
    return low, high


def own_codes(links, first, blocks):
    codes = links[:, 1] * KINDS + links[:, 2]
    hit = links[:, 0][None, :] == (first + jnp.arange(blocks, dtype=jnp.int32))[:, None]
    low = jnp.min(jnp.where(hit, codes[None, :], UBLOCKS * KINDS), axis=1)
    high = jnp.max(jnp.where(hit, codes[None, :], -1), axis=1)
    return low, high


def chosen_codes(chosen):
    block = chosen // BLOCK
    codes = jnp.stack([block // 32, block % 32, chosen % BLOCK], axis=1)
    return jnp.pad(codes.astype(jnp.bfloat16), ((0, 0), (0, BLOCK - 3)))


def column_tile(hidden_cat, chosen):
    rows, columns = hidden_cat.shape
    parts = hidden_cat.reshape(rows, 8, columns // 8).transpose(1, 0, 2)
    codes = jnp.broadcast_to(chosen_codes(chosen)[None], (8, rows, BLOCK))
    tile = lax.all_to_all(jnp.concatenate([parts, codes], axis=2), GROUP, 0, 0, tiled=True)
    tile = tile.reshape(8 * rows, -1)
    return tile[:, :-BLOCK], tile[:, -BLOCK:]


def chunk_tensor(y, k):
    return lax.rem(y + 4 - k, 4)


def ensemble_kernel(
    tile_ref,
    code_ref,
    own_ref,
    low_ref,
    high_ref,
    weights_ref,
    prior_ref,
    q_head_ref,
    l_head_ref,
    out_ref,
    lik_ref,
    held,
    codes,
    q_head,
    l_head,
    found,
    parts,
    sums,
    lines,
    sent,
    got,
    terms,
    mixed_out,
    mixed_in,
    lik_out,
    lik_in,
    owned_out,
    owned_in,
    turned,
    head_sem,
    y_send,
    y_recv,
    z_send,
    z_recv,
    code_send,
    code_recv,
    core_send,
    core_recv,
    x_send,
    x_recv,
    row_send,
    row_recv,
    swap_send,
    swap_recv,
    mix_send,
    mix_recv,
    end_send,
    end_recv,
):
    z, y, c, x = (lax.axis_index(name) for name in ("vocab_0", "vocab_1", "vocab_2", "width"))
    other = 1 - c
    z_next = (lax.rem(z + 1, 16), lax.rem(z + 15, 16))
    x_next = (lax.rem(x + 1, 4), lax.rem(x + 3, 4))
    chunk = tile_ref.shape[1]
    f32, bf16 = jnp.float32, jnp.bfloat16

    def to(src, dst, send, recv, device):
        return pltpu.make_async_remote_copy(
            src_ref=src,
            dst_ref=dst,
            send_sem=send,
            recv_sem=recv,
            device_id=device,
            device_id_type=pl.DeviceIdType.MESH,
        )

    def plane(way, step):
        return lax.rem(z + 16 - step, 16) if way == 0 else lax.rem(z + step, 16)

    def pair(group):
        return lax.rem(z + 16 - group, 16), lax.rem(z + jnp.where(group == 8, 0, group), 16)

    def z_copy(way, k, step, src=None):
        place = held.at[plane(way, step - 1), c, chunk_tensor(y, k)]
        src = place if src is None else src
        return to(src, place, z_send.at[way, k, step], z_recv.at[way, k, step], {"vocab_0": z_next[way]})

    def z_arrival(way, k, step):
        place = held.at[plane(way, step), c, chunk_tensor(y, k)]
        return to(place, place, z_send.at[way, k, step], z_recv.at[way, k, step], {"vocab_0": z_next[way]})

    def code_copy(way, step, at):
        place = codes.at[plane(way, at)]
        return to(place, place, code_send.at[way, step], code_recv.at[way, step], {"vocab_0": z_next[way]})

    def core_copy(way, step, at, core):
        place = held.at[at, core]
        return to(place, place, core_send.at[way, step], core_recv.at[way, step], {"vocab_2": other})

    def x_copy(hop, way, group, src):
        dst = sums.at[hop, way, group]
        send, recv = x_send.at[hop, way, group], x_recv.at[hop, way, group]
        return to(src, dst, send, recv, {"width": x_next[way]})

    def x_class(way, hop):
        return lax.rem(x + 7 - hop, 4) if way == 0 else lax.rem(x + 1 + hop, 4)

    def row_copy(dz, dy, at_z, at_y):
        send, recv = row_send.at[dz, dy], row_recv.at[dz, dy]
        device = {"vocab_0": at_z, "vocab_1": at_y}
        return to(sent.at[at_z, at_y], got.at[c, z, y], send, recv, device)

    def end_copy(dz, dy, at_z, at_y):
        send, recv = end_send.at[dz, dy], end_recv.at[dz, dy]
        device = {"vocab_0": at_z, "vocab_1": at_y}
        return to(owned_out.at[at_z, at_y], owned_in.at[z, y], send, recv, device)

    def mix_copies(dx, t):
        to_x = lax.rem(x + dx, 4)
        send, recv = mix_send.at[t, dx], mix_recv.at[t, dx]
        if t == 2:
            return to(lik_out, lik_in.at[x], send, recv, {"width": to_x})
        return to(mixed_out.at[t, to_x], mixed_in.at[t, x], send, recv, {"width": to_x})

    head_copies = (
        pltpu.make_async_copy(q_head_ref, q_head, head_sem.at[0]),
        pltpu.make_async_copy(l_head_ref, l_head, head_sem.at[1]),
    )
    for copy in head_copies:
        copy.start()
    barrier = pltpu.get_barrier_semaphore()
    peers = [{"vocab_0": z_next[0]}, {"vocab_0": z_next[1]}, {"vocab_2": other}]
    peers += [{"vocab_1": lax.rem(y + step, 4)} for step in (1, 2, 3)]
    peers += [{"width": lax.rem(x + step, 4)} for step in (1, 2, 3)]
    for device in peers:
        pl.semaphore_signal(barrier, inc=1, device_id=device, device_id_type=pl.DeviceIdType.MESH)
    pl.semaphore_wait(barrier, len(peers))

    y_copies = [
        to(
            tile_ref,
            held.at[z, c, y],
            y_send.at[k],
            y_recv.at[k],
            {"vocab_1": lax.rem(y + k + 1, 4)},
        )
        for k in range(3)
    ]
    for copy in y_copies:
        copy.start()
    for way in range(2):
        z_copy(way, 0, 1, tile_ref).start()
        send, recv = code_send.at[way, 1], code_recv.at[way, 1]
        to(code_ref, codes.at[z], send, recv, {"vocab_0": z_next[way]}).start()
    held[z, c, y] = tile_ref[...]
    codes[z] = code_ref[...]
    lines[...] = jnp.zeros(lines.shape, f32)
    for k in range(1, 4):
        place = held.at[z, c, chunk_tensor(y, k)]
        to(place, place, y_send.at[k - 1], y_recv.at[k - 1], {"vocab_1": lax.rem(y + k, 4)}).wait_recv()
        for way in range(2):
            z_copy(way, k, 1).start()
    core_copy(1, 8, z, c).start()
    for copy in head_copies:
        copy.wait()

    def multiply(group, model):
        low, high = pair(group)
        head, first = ((q_head, 0), (l_head, QB_DEV))[model]
        total = None
        for half in range(2):
            rows = jnp.concatenate(
                [held[at, half, 2 * model + s] for s in range(2) for at in (low, high)], axis=0
            )
            term = lax.dot_general(
                rows,
                head[:, half * chunk : (half + 1) * chunk],
                (((1,), (1,)), ((), ())),
                preferred_element_type=f32,
            )
            total = term if total is None else total + term
        for b in range(head.shape[0] // BLOCK):
            found[first + b] = total[:, b * BLOCK : (b + 1) * BLOCK]

    def split_rows(group):
        for b in range(B_DEV):
            for s in range(2):
                for turn in range(4):
                    rows = found[b, pl.ds(32 * s + turn, 8, stride=4), :]
                    parts[group, s, turn, :, b * BLOCK : (b + 1) * BLOCK] = rows

    def chosen_weights(low, high):
        for n, at in enumerate((low, high)):
            turned[16 * n : 16 * (n + 1), :] = codes[at].astype(f32)
        picked = turned[pl.ds(x, 8, stride=4), :]
        block = picked[:, 0:1] * 32.0 + picked[:, 1:2]
        lane = lax.broadcasted_iota(jnp.int32, (8, BLOCK), 1)
        one_hot = jnp.where(picked[:, 2:3] == lane.astype(f32), 1.0, 0.0).astype(bf16)
        weight = [jnp.zeros((8, BLOCK), f32) for _ in range(B_DEV)]
        for kind in range(KINDS):
            column = lax.dot_general(
                one_hot, weights_ref[kind], (((1,), (1,)), ((), ())), preferred_element_type=f32
            )
            code = block * KINDS + kind
            for b in range(B_DEV):
                count = jnp.where(own_ref[b : b + 1, :] == code, 1.0, 0.0) + jnp.where(
                    own_ref[16 + b : 17 + b, :] == code, 1.0, 0.0
                )
                weight[b] += count * column
        return weight

    def message_rows(group, totals):
        low, high = pair(group)
        weight = chosen_weights(low, high)
        spans = ((0, QB_DEV), (QB_DEV, B_DEV))
        values = []
        for s in range(2):
            for first, last in spans:
                part = totals[s][:, first * BLOCK : last * BLOCK]
                top = jnp.max(part, axis=1, keepdims=True)
                powers = jnp.exp(part - top)
                values += [top, jnp.sum(powers, axis=1, keepdims=True)]
                pieces = [powers[:, b * BLOCK : (b + 1) * BLOCK] for b in range(last - first)]
                if s == 0:
                    value = sum(piece * weight[first + b] for b, piece in enumerate(pieces))
                    values.append(jnp.sum(value, axis=1, keepdims=True))
                else:
                    for b, piece in enumerate(pieces):
                        for n, at in enumerate((low, high)):
                            lines[pl.ds(at * 64 + first + b, 4, stride=16), :] = piece[4 * n : 4 * n + 4]
        lane = lax.broadcasted_iota(jnp.int32, (8, BLOCK), 1)
        rest = jnp.zeros((8, BLOCK), f32)
        for n, value in enumerate(values):
            rest = jnp.where(lane == n, value, rest)
        for row in range(3):
            part = rest.astype(bf16).astype(f32)
            rest = rest - part
            for n, at in enumerate((low, high)):
                lines[pl.ds(at * 64 + B_DEV + row, 4, stride=16), :] = part[4 * n : 4 * n + 4]
        for at in (low, high):
            rows = lines[pl.ds(pl.multiple_of(at * 64, 64), 64), :]
            sent[at] = rows.astype(bf16).reshape(4, 16, BLOCK)
        for way, at in enumerate((low, high)):
            for dy in range(4):
                to_y = lax.rem(y + dy, 4)
                if way == 0:
                    row_copy(16 - group, dy, at, to_y).start()
                else:
                    dz = jnp.where(group == 8, 0, group)
                    if dy:
                        row_copy(dz, dy, at, to_y).start()
                    else:

                        @pl.when(group < 8)
                        def _():
                            row_copy(dz, dy, at, to_y).start()

    def step(it, carry):
        def on_group(group, run):
            pl.when((group >= 1) & (group <= 8))(run)

        def forward(k):
            for way in range(2):
                last = 8 if (k < 2) == (way == 0) else 7

                @pl.when(it <= last)
                def _():
                    z_arrival(way, k, it).wait_recv()

                @pl.when(it < last)
                def _():
                    z_copy(way, k, it + 1).start()

        def first_hop():
            group = it - 1
            split_rows(group)
            for way in range(2):
                x_copy(0, way, group, parts.at[group, way, x_class(way, 0)]).start()

        def next_hop(hop):
            group = it - 1 - hop
            for way in range(2):
                place = sums.at[hop - 1, way, group]
                x_copy(hop - 1, way, group, place).wait_recv()
                place[...] = place[...] + parts[group, way, x_class(way, hop)]
                x_copy(hop, way, group, place).start()

        def last_hop():
            group = it - 4
            totals = []
            for way in range(2):
                place = sums.at[2, way, group]
                x_copy(2, way, group, place).wait_recv()
                totals.append(place[...] + parts[group, way, x])
            message_rows(group, totals)

        def arrived():
            low, high = pair(it - 1)
            core_copy(0, it - 1, low, other).wait_recv()
            core_copy(1, it - 1, high, other).wait_recv()
            multiply(it - 1, 0)

        forward(0)
        on_group(it - 1, arrived)
        forward(1)
        on_group(it - 1, lambda: multiply(it - 1, 1))
        forward(2)
        on_group(it - 1, first_hop)
        on_group(it - 2, lambda: next_hop(1))
        on_group(it - 3, lambda: next_hop(2))
        forward(3)
        for way in range(2):
            last = 8 - way

            @pl.when(it <= last)
            def _():
                core_copy(way, it, plane(way, it), c).start()
                code_copy(way, it, it).wait_recv()

            @pl.when(it < last)
            def _():
                code_copy(way, it + 1, it).start()

        on_group(it - 4, last_hop)
        return carry

    lax.fori_loop(1, 13, step, 0)

    got[c, z, y] = sent[z, y]

    def others(run):
        def visit(i, carry):
            dz, dy = i // 4, lax.rem(i, 4)
            run(dz, dy)
            return carry

        lax.fori_loop(1, 64, visit, 0)

    def row_arrival(dz, dy):
        at_z, at_y = lax.rem(z + 16 - dz, 16), lax.rem(y + 4 - dy, 4)
        place = got.at[c, at_z, at_y]
        to(place, place, row_send.at[dz, dy], row_recv.at[dz, dy], {"vocab_0": at_z}).wait_recv()

    others(row_arrival)
    swap = to(got.at[c], got.at[c], swap_send, swap_recv, {"vocab_2": other})
    swap.start()
    to(got.at[other], got.at[other], swap_send, swap_recv, {"vocab_2": other}).wait_recv()
    terms[...] = got[...].reshape(terms.shape).astype(f32)

    stats = terms[pl.ds(B_DEV, 128, stride=16), :]
    for row in range(1, 3):
        stats = stats + terms[pl.ds(B_DEV + row, 128, stride=16), :]
    highest = jnp.max(stats, axis=0, keepdims=True)

    def share(n):
        factor = jnp.exp(stats[:, n : n + 1] - highest[:, n : n + 1])
        return factor, jnp.sum(factor * stats[:, n + 1 : n + 2], axis=0, keepdims=True)

    masses = []
    for model in range(2):
        factor, total = share(3 * model)
        value = jnp.sum(factor * stats[:, 3 * model + 2 : 3 * model + 3], axis=0, keepdims=True)
        value = 0.5 * value / total
        prior = prior_ref[model : model + 1, 0:1]
        masses.append(prior * ((1.0 - SMOOTHING) * value + UNIFORM))
    together = masses[0] + masses[1]
    lik_out[...] = jnp.broadcast_to(jnp.log(together), lik_out.shape)
    for dx in range(1, 4):
        mix_copies(dx, 2).start()
    scales = []
    for model in range(2):
        factor, total = share(6 + 2 * model)
        scales.append(factor * ((masses[model] / together) * 0.5 / total))
    for b in range(B_DEV):
        rows = terms[pl.ds(b, 128, stride=16), :]
        scaled = rows * scales[0 if b < QB_DEV else 1]
        found_b = scaled.astype(bf16)
        sent_b = (b * 128, (b + 1) * 128)
        turned[sent_b[0] : sent_b[1], :] = found_b.astype(f32)

    spot = lax.broadcasted_iota(jnp.int32, (256, BLOCK), 0)
    first = (16 * lax.rem(spot, 64) + 8 * c + 2 * (spot // 64)) * KINDS
    for t in range(2):
        mixed = jnp.zeros((256, BLOCK), f32)
        for kind in range(KINDS):
            code = first + (t * KINDS + kind)
            total = jnp.zeros((256, BLOCK), f32)
            for b in range(B_DEV):
                hits = jnp.where(low_ref[b : b + 1, :] == code, 1.0, 0.0) + jnp.where(
                    high_ref[b : b + 1, :] == code, 1.0, 0.0
                )
                total += jnp.dot(
                    hits.astype(bf16),
                    turned[b * 128 : (b + 1) * 128, :].astype(bf16),
                    preferred_element_type=f32,
                )
            mixed += jnp.dot(total.astype(bf16), weights_ref[kind], preferred_element_type=f32)
        mixed_out[t] = mixed.astype(bf16).reshape(4, 64, BLOCK)
        for dx in range(1, 4):
            mix_copies(dx, t).start()
        mixed_in[t, x] = mixed_out[t, x]
    lik_in[x] = lik_out[...]
    for dx in range(1, 4):
        from_x = lax.rem(x + 4 - dx, 4)
        for t in range(3):
            place = lik_in.at[from_x] if t == 2 else mixed_in.at[t, from_x]
            to(place, place, mix_send.at[t, dx], mix_recv.at[t, dx], {"width": from_x}).wait_recv()
    for t in range(2):
        for w in range(4):
            lines[pl.ds(w * 2 + t, 64, stride=8), :] = mixed_in[t, w].astype(f32)
    owned_out[...] = lines[0:512, :].reshape(16, 4, 8, BLOCK).astype(bf16)

    def end_start(dz, dy):
        end_copy(dz, dy, lax.rem(z + dz, 16), lax.rem(y + dy, 4)).start()

    def end_arrival(dz, dy):
        at_z, at_y = lax.rem(z + 16 - dz, 16), lax.rem(y + 4 - dy, 4)
        place = owned_in.at[at_z, at_y]
        to(place, place, end_send.at[dz, dy], end_recv.at[dz, dy], {"vocab_0": at_z}).wait_recv()

    others(end_start)
    owned_in[z, y] = owned_out[z, y]
    lik_ref[...] = lik_in[...]
    others(end_arrival)
    turned[0:512, :] = owned_in[...].astype(f32).reshape(512, BLOCK)
    for t in range(2):
        rows = turned[pl.ds(t, 256, stride=2), :]
        out_ref[:, t * BLOCK : (t + 1) * BLOCK] = jnp.log((1.0 - SMOOTHING) * rows + UNIFORM)

    for copy in y_copies:
        copy.wait_send()

    def drain(it, carry):
        for way in range(2):
            for k in range(4):
                last = 8 if (k < 2) == (way == 0) else 7

                @pl.when(it <= last)
                def _():
                    z_copy(way, k, it).wait_send()

            last = 8 - way

            @pl.when(it <= last)
            def _():
                code_copy(way, it, it).wait_send()

            core_copy(way, it, z, c).wait_send()
            for hop in range(3):
                x_copy(hop, way, it, sums.at[0, way, it]).wait_send()
        return carry

    lax.fori_loop(1, 9, drain, 0)

    def sent_all(dz, dy):
        at_z, at_y = lax.rem(z + dz, 16), lax.rem(y + dy, 4)
        row_copy(dz, dy, at_z, at_y).wait_send()
        end_copy(dz, dy, at_z, at_y).wait_send()

    others(sent_all)
    swap.wait_send()
    for dx in range(1, 4):
        for t in range(3):
            mix_copies(dx, t).wait_send()


def ensemble(tile, code, own, low, high, weights, prior, q_head, l_head):
    rows, chunk = tile.shape
    entries = q_head.shape[0] + l_head.shape[0]
    vmem = pl.BlockSpec(memory_space=pltpu.VMEM)
    dma = pltpu.SemaphoreType.DMA
    bf16, f32 = jnp.bfloat16, jnp.float32
    return pl.pallas_call(
        ensemble_kernel,
        out_shape=(
            jax.ShapeDtypeStruct((256, 2 * BLOCK), f32),
            jax.ShapeDtypeStruct((4, 8, BLOCK), f32),
        ),
        in_specs=[*[vmem] * 7, *[pl.BlockSpec(memory_space=pltpu.HBM)] * 2],
        out_specs=(vmem, vmem),
        scratch_shapes=[
            pltpu.VMEM((16, 2, 4, rows, chunk), bf16),
            pltpu.VMEM((16, rows, BLOCK), bf16),
            pltpu.VMEM(q_head.shape, bf16),
            pltpu.VMEM(l_head.shape, bf16),
            pltpu.VMEM((B_DEV, 4 * rows, BLOCK), f32),
            pltpu.VMEM((9, 2, 4, 8, entries), f32),
            pltpu.VMEM((3, 2, 9, 8, entries), f32),
            pltpu.VMEM((16 * 64, BLOCK), f32),
            pltpu.VMEM((16, 4, 16, BLOCK), bf16),
            pltpu.VMEM((2, 16, 4, 16, BLOCK), bf16),
            pltpu.VMEM((2048, BLOCK), f32),
            pltpu.VMEM((2, 4, 64, BLOCK), bf16),
            pltpu.VMEM((2, 4, 64, BLOCK), bf16),
            pltpu.VMEM((8, BLOCK), f32),
            pltpu.VMEM((4, 8, BLOCK), f32),
            pltpu.VMEM((16, 4, 8, BLOCK), bf16),
            pltpu.VMEM((16, 4, 8, BLOCK), bf16),
            pltpu.VMEM((B_DEV * BLOCK, BLOCK), f32),
            dma((2,)),
            *[dma((3,))] * 2,
            *[dma((2, 4, 9))] * 2,
            *[dma((2, 9))] * 2,
            *[dma((2, 9))] * 2,
            *[dma((3, 2, 9))] * 2,
            *[dma((16, 4))] * 2,
            *[dma(())] * 2,
            *[dma((3, 4))] * 2,
            *[dma((16, 4))] * 2,
        ],
        compiler_params=pltpu.CompilerParams(
            collective_id=0, has_side_effects=True, vmem_limit_bytes=56 * 1024 * 1024
        ),
        cost_estimate=pl.CostEstimate(flops=3 * 10**10, bytes_accessed=10**7, transcendentals=0),
    )(tile, code, own, low, high, weights, prior, q_head, l_head)


def by_source(codes, per_device):
    return codes.reshape(-1, 2, per_device).transpose(2, 1, 0).reshape(per_device, -1)


def local(
    qwen_hidden,
    qwen_next_hidden,
    llama_hidden,
    llama_next_hidden,
    qwen_head,
    llama_head,
    align_weights,
    qwen_links,
    llama_links,
    union_order,
    chosen,
    model_weight,
):
    core = lax.axis_index("vocab_2")
    owner = lax.axis_index(VOCAB)
    hidden_cat = jnp.concatenate(
        [qwen_hidden, qwen_next_hidden, llama_hidden, llama_next_hidden], axis=1
    )
    tile, code = column_tile(hidden_cat, chosen)
    q_low, q_high = link_codes(qwen_links, union_order, qwen_links.shape[0] // 2)
    l_low, l_high = link_codes(llama_links, union_order, llama_links.shape[0] // 2)
    low, high = (
        jnp.concatenate([by_source(q, QB_DEV), by_source(l, LB_DEV)])
        for q, l in ((q_low, l_low), (q_high, l_high))
    )
    q_own = own_codes(qwen_links, owner * QB_DEV, QB_DEV)
    l_own = own_codes(llama_links, owner * LB_DEV, LB_DEV)
    own = jnp.concatenate([jnp.pad(jnp.concatenate(pair), (0, 16 - B_DEV)) for pair in zip(q_own, l_own)])
    own = jnp.broadcast_to(own.astype(jnp.float32)[:, None], (32, BLOCK))
    prior = model_weight / (model_weight[0] + model_weight[1])
    prior = jnp.broadcast_to(prior[:, None], (2, BLOCK))
    next_logprob, logliks = ensemble(
        tile, code, own, low, high, align_weights, prior, qwen_head, llama_head
    )
    return next_logprob, lax.dynamic_slice(logliks[:, 0, 0], (2 * core,), (2,))


def solution(mesh):
    torus = Mesh(
        mesh.devices.reshape(16, 4, 2, mesh.shape["width"]),
        ("vocab_0", "vocab_1", "vocab_2", "width"),
    )
    return jax.shard_map(
        local,
        mesh=torus,
        in_specs=(*[P(VOCAB, "width")] * 6, P(), P(), P(), P(), P(VOCAB), P()),
        out_specs=(P(None, (*VOCAB, "width")), P(VOCAB)),
        check_vma=False,
    )
```
